32 devices in a mesh: rep: 2 (over core), row: 8 (over z, x), col: 2 (over y).
Axes of the slice: x: 2, y: 2, z: 4, core: 2. Of those that a mesh axis runs over, the one named last changes fastest.
Arguments:
- sources: float32 [2, 384, 384, 384], P('rep', 'col', 'row'), may hold values from -6 to 6
Outputs:
- potential: float32 [384, 384, 384], P(('rep', 'col'), 'row')
The draws below stay inside these ranges and needn't reach their ends.
All inputs are finite; a program needn't handle non-finite values.
Results may differ from the reference program's by a relative error of at most 0.000096.
Values sent between devices are 32-bit elements; how exact they have to be, the bound alone decides.
A program may use at most 128 MiB of HBM per device.

```python
import jax
import jax.numpy as jnp

NA = 384
NB = 384
NC = 384


def draw_sources(key, part):
    noise_key = jax.random.fold_in(key, 0)
    return jnp.clip(jax.random.normal(noise_key, (2, NA, NB, NC), jnp.float32), -6.0, 6.0)


def setup_inputs(seed: int = 0) -> dict:
    streams_of = jax.random.split(jax.random.key(seed), 2)
    return {
        "sources": draw_sources(jax.random.fold_in(streams_of[1], 71), 0),
    }


def laplace_eigen(length):
    modes = jnp.arange(length, dtype=jnp.int32).astype(jnp.float32)
    sines = jnp.sin(modes * (jnp.pi / length))
    return 4.0 * sines * sines


def reference(sources):
    density = sources[0] + sources[1]
    spectrum = jnp.fft.fftn(density)
    eigen_a = laplace_eigen(NA)
    eigen_b = laplace_eigen(NB)
    eigen_c = laplace_eigen(NC)
    total = eigen_a[:, None, None] + eigen_b[None, :, None] + eigen_c[None, None, :] + 0.001
    green = 1.0 / total
    potential = jnp.real(jnp.fft.ifftn(spectrum * green))
    return potential.astype(jnp.float32)
```

```python
import functools
import math

import jax
import jax.numpy as jnp
import numpy as np
from jax import lax
from jax.experimental import pallas as pl
from jax.experimental.pallas import tpu as pltpu
from jax.sharding import PartitionSpec as P

NA = 384
NB = 384
NC = 384


highest = lax.Precision.HIGHEST


def wave_tables(freq_index, position, length):
    turns = freq_index[:, None] * position[None, :] % length
    angle = turns.astype(jnp.float32) * (2.0 * math.pi / length)
    return (jnp.cos(angle), jnp.sin(angle))


def matmul_high(first_matrix, second_matrix):
    return jnp.dot(
        first_matrix, second_matrix, precision=highest, preferred_element_type=jnp.float32
    )


def leading_contract(first_matrix, second_matrix):
    return lax.dot_general(
        first_matrix,
        second_matrix,
        (((0,), (0,)), ((), ())),
        precision=highest,
        preferred_element_type=jnp.float32,
    )


def trailing_contract(first_matrix, second_matrix):
    return lax.dot_general(
        first_matrix,
        second_matrix,
        (((1,), (1,)), ((), ())),
        precision=highest,
        preferred_element_type=jnp.float32,
    )


def table_against_rows(table, flat_rows):
    return lax.dot_general(
        table,
        flat_rows,
        (((0,), (1,)), ((), ())),
        precision=highest,
        preferred_element_type=jnp.float32,
    )


def laplace_eigen(wave_index, length):
    sines = jnp.sin(wave_index.astype(jnp.float32) * (math.pi / length))
    return 4.0 * sines * sines


def mirror_modes(values, axis_number):
    return jnp.roll(jnp.flip(values, axis_number), 1, axis_number)


def body(sources):
    partial_value = sources[0]
    density = lax.psum_scatter(partial_value, "rep", scatter_dimension=0, tiled=True)
    slab_rows, line_rows, length_c = density.shape
    rep_count = lax.axis_size("rep")
    col_count = lax.axis_size("col")
    third_len = NC // 2
    freq_block = third_len // (rep_count * col_count)
    half_first = NA // 2
    modes_first = jnp.arange(NA, dtype=jnp.int32)
    modes_second = jnp.arange(NB, dtype=jnp.int32)
    modes_third = jnp.arange(NC, dtype=jnp.int32)
    modes_spec = jnp.arange(third_len, dtype=jnp.int32)
    parity = (1 - 2 * (modes_third % 2)).astype(jnp.float32)
    owner_zero = (lax.axis_index("rep") == 0) & (lax.axis_index("col") == 0)
    flat_density = density.reshape(slab_rows * line_rows, NC)
    cos_spec, sin_spec = wave_tables(modes_spec, modes_third, NC)
    sin_spec = jnp.where(modes_spec[:, None] == 0, -parity[None, :], sin_spec)
    real_third = trailing_contract(flat_density, cos_spec).reshape(slab_rows, line_rows, third_len)
    imag_third = (-trailing_contract(flat_density, sin_spec)).reshape(
        slab_rows, line_rows, third_len
    )
    group_first = modes_first // slab_rows
    first_index = (
        group_first % col_count * (rep_count * slab_rows)
        + group_first // col_count * slab_rows
        + modes_first % slab_rows
    )
    cos_first, sin_first = wave_tables(first_index, modes_first, NA)
    real_in = lax.all_to_all(real_third, ("rep", "col"), split_axis=2, concat_axis=0, tiled=True)
    imag_in = lax.all_to_all(imag_third, ("rep", "col"), split_axis=2, concat_axis=0, tiled=True)
    count = real_in.shape[1]
    flat_real = real_in.reshape(NA, count * freq_block)
    flat_imag = imag_in.reshape(NA, count * freq_block)
    real_out = leading_contract(flat_real, cos_first) + leading_contract(flat_imag, sin_first)
    imag_out = leading_contract(flat_imag, cos_first) - leading_contract(flat_real, sin_first)
    real_first = real_out.reshape(count, freq_block, NA)
    imag_first = imag_out.reshape(count, freq_block, NA)
    packed_r = real_first[:, 0, :]
    packed_i = imag_first[:, 0, :]
    mirror_r = mirror_modes(packed_r, 1)
    mirror_i = mirror_modes(packed_i, 1)
    zero_r = 0.5 * (packed_r + mirror_r)
    zero_i = 0.5 * (packed_i - mirror_i)
    top_r = 0.5 * (packed_i + mirror_i)
    top_i = -0.5 * (packed_r - mirror_r)
    edge_modes = ((modes_first == 0) | (modes_first == half_first))[None, :]
    lower_modes = (modes_first <= half_first)[None, :]
    new_r = jnp.where(lower_modes, zero_r, top_r)
    new_i = jnp.where(edge_modes, top_r, jnp.where(lower_modes, zero_i, top_i))
    real_first = real_first.at[:, 0, :].set(jnp.where(owner_zero, new_r, packed_r))
    imag_first = imag_first.at[:, 0, :].set(jnp.where(owner_zero, new_i, packed_i))
    cos_second, sin_second = wave_tables(modes_second, modes_second, NB)
    real_in = lax.all_to_all(real_first, "row", split_axis=2, concat_axis=0, tiled=True)
    imag_in = lax.all_to_all(imag_first, "row", split_axis=2, concat_axis=0, tiled=True)
    count = real_in.shape[1]
    tail = real_in.shape[2]
    flat_real = real_in.reshape(NB, count * tail)
    flat_imag = imag_in.reshape(NB, count * tail)
    real_out = matmul_high(cos_second, flat_real) + matmul_high(sin_second, flat_imag)
    imag_out = matmul_high(cos_second, flat_imag) - matmul_high(sin_second, flat_real)
    real_second = real_out.reshape(NB, count, tail)
    imag_second = imag_out.reshape(NB, count, tail)
    freq_rows = real_second.shape[2]
    first_freqs = lax.axis_index("row") * freq_rows + jnp.arange(freq_rows, dtype=jnp.int32)
    third_freqs = (
        lax.axis_index("rep") * col_count + lax.axis_index("col")
    ) * freq_block + jnp.arange(freq_block, dtype=jnp.int32)
    scale_all = 1.0 / (NA * NB * NC)
    eigen_second = laplace_eigen(modes_second, NB)
    eigen_first = laplace_eigen(first_freqs, NA)
    total = (
        eigen_second[:, None, None]
        + laplace_eigen(third_freqs, NC)[None, :, None]
        + eigen_first[None, None, :]
        + 0.001
    )
    green = 1.0 / total * scale_all
    filt_real = real_second * green
    filt_imag = imag_second * green
    wave_r = real_second[:, 0, :]
    wave_i = imag_second[:, 0, :]
    green_zero = green[:, 0, :]
    green_top = 1.0 / (eigen_second[:, None] + 4.0 + eigen_first[None, :] + 0.001) * scale_all
    mean_green = 0.5 * (green_zero + green_top)
    diff_green = 0.5 * (green_zero - green_top)
    mixed_r = mean_green * wave_r + diff_green * mirror_modes(wave_r, 0)
    mixed_i = mean_green * wave_i - diff_green * mirror_modes(wave_i, 0)
    lower_freqs = ((first_freqs > 0) & (first_freqs < half_first))[None, :]
    upper_freqs = (first_freqs > half_first)[None, :]
    slot_r = jnp.where(
        lower_freqs, green_zero * wave_r, jnp.where(upper_freqs, green_top * wave_r, mixed_r)
    )
    slot_i = jnp.where(
        lower_freqs, green_zero * wave_i, jnp.where(upper_freqs, green_top * wave_i, mixed_i)
    )
    filt_real = filt_real.at[:, 0, :].set(jnp.where(owner_zero, slot_r, filt_real[:, 0, :]))
    filt_imag = filt_imag.at[:, 0, :].set(jnp.where(owner_zero, slot_i, filt_imag[:, 0, :]))
    flat_real = filt_real.reshape(NB, freq_block * freq_rows)
    flat_imag = filt_imag.reshape(NB, freq_block * freq_rows)
    real_back = (matmul_high(cos_second, flat_real) - matmul_high(sin_second, flat_imag)).reshape(
        NB, freq_block, freq_rows
    )
    imag_back = (matmul_high(cos_second, flat_imag) + matmul_high(sin_second, flat_real)).reshape(
        NB, freq_block, freq_rows
    )
    cos_inverse, sin_inverse = wave_tables(modes_first, modes_first, NA)
    real_in = lax.all_to_all(real_back, "row", split_axis=0, concat_axis=2, tiled=True)
    imag_in = lax.all_to_all(imag_back, "row", split_axis=0, concat_axis=2, tiled=True)
    b_count = real_in.shape[0]
    count = real_in.shape[1]
    flat_real_in = real_in.reshape(b_count * count, NA)
    flat_imag_in = imag_in.reshape(b_count * count, NA)
    real_out = table_against_rows(cos_inverse, flat_real_in) - table_against_rows(
        sin_inverse, flat_imag_in
    )
    imag_out = table_against_rows(cos_inverse, flat_imag_in) + table_against_rows(
        sin_inverse, flat_real_in
    )
    real_lines = real_out.reshape(NA, b_count, count)
    imag_lines = imag_out.reshape(NA, b_count, count)
    field_r = real_lines[:, :, 0]
    field_i = imag_lines[:, :, 0]
    spec_r = (matmul_high(cos_inverse, field_r) + matmul_high(sin_inverse, field_i)) * (1.0 / NA)
    spec_i = (matmul_high(cos_inverse, field_i) - matmul_high(sin_inverse, field_r)) * (1.0 / NA)
    mirror_r = mirror_modes(spec_r, 0)
    mirror_i = mirror_modes(spec_i, 0)
    lower_lines = ((modes_first > 0) & (modes_first < half_first))[:, None]
    upper_lines = (modes_first > half_first)[:, None]
    joined_r = jnp.where(
        lower_lines, spec_r + mirror_i, jnp.where(upper_lines, mirror_r - spec_i, spec_r)
    )
    joined_i = jnp.where(
        lower_lines, spec_i + mirror_r, jnp.where(upper_lines, spec_r - mirror_i, spec_i)
    )
    rebuilt_r = matmul_high(cos_inverse, joined_r) - matmul_high(sin_inverse, joined_i)
    rebuilt_i = matmul_high(cos_inverse, joined_i) + matmul_high(sin_inverse, joined_r)
    real_lines = real_lines.at[:, :, 0].set(jnp.where(owner_zero, rebuilt_r, field_r))
    imag_lines = imag_lines.at[:, :, 0].set(jnp.where(owner_zero, rebuilt_i, field_i))
    cos_final, sin_final = wave_tables(modes_spec, modes_third, NC)
    weight = jnp.where(modes_spec == 0, 1.0, 2.0).astype(jnp.float32)[:, None]
    cos_final = weight * cos_final
    sin_final = jnp.where(modes_spec[:, None] == 0, -parity[None, :], 2.0 * sin_final)
    real_in = lax.all_to_all(real_lines, ("rep", "col"), split_axis=0, concat_axis=2, tiled=True)
    imag_in = lax.all_to_all(imag_lines, ("rep", "col"), split_axis=0, concat_axis=2, tiled=True)
    a_count = real_in.shape[0]
    count = real_in.shape[1]
    spec_len = real_in.shape[2]
    flat_real_in = real_in.reshape(a_count * count, spec_len)
    flat_imag_in = imag_in.reshape(a_count * count, spec_len)
    result = matmul_high(flat_real_in, cos_final) - matmul_high(flat_imag_in, sin_final)
    return result.reshape(a_count, count, NC)


def slab_tables(length):
    turns = np.outer(np.arange(length), np.arange(length)) % length
    angle = turns * (2.0 * np.pi / length)
    table = np.cos(angle) + np.sin(angle)
    high = table.astype(jnp.bfloat16)
    low = (table - high.astype(np.float64)).astype(jnp.bfloat16)
    return jnp.asarray(high), jnp.asarray(low)


def eigen_values(length):
    sines = np.sin(np.arange(length) * (np.pi / length))
    return (4.0 * sines * sines).astype(np.float32)


def halves(value):
    high = value.astype(jnp.bfloat16)
    low = (value - high.astype(jnp.float32)).astype(jnp.bfloat16)
    return high, low


def dot_f32(left, right):
    return jnp.dot(left, right, preferred_element_type=jnp.float32)


def times_table(value, high, low):
    top, rest = halves(value)
    return dot_f32(top, high) + dot_f32(top, low) + dot_f32(rest, high)


def table_times(high, low, value):
    top, rest = halves(value)
    return dot_f32(high, top) + dot_f32(low, top) + dot_f32(high, rest)


def decay_of(shift):
    root = jnp.sqrt(shift * (shift + 4.0))
    return 2.0 / (2.0 + shift + root), root


def forward_kernel(ah, al, ch, cl, eig_a, eig_c, x_ref, z_ref, up_ref, down_ref, rho, power):
    step = pl.program_id(0)
    lines = times_table(x_ref[0], ch[...], cl[...])
    modes = table_times(ah[...], al[...], lines)
    z_ref[0] = modes

    @pl.when(step == 0)
    def _():
        rho[...] = decay_of(eig_a[...] + eig_c[...] + 0.001)[0]
        power[...] = rho[...]
        up_ref[...] = modes
        down_ref[...] = modes

    @pl.when(step > 0)
    def _():
        up_ref[...] = modes + rho[...] * up_ref[...]
        down_ref[...] = down_ref[...] + power[...] * modes
        power[...] = power[...] * rho[...]


def backward_kernel(scale, ah, al, ch, cl, eig_a, eig_c, z_ref, carry, out_ref, rho, gain, run, back):
    step = pl.program_id(0)
    count = z_ref.shape[0]

    @pl.when(step == 0)
    def _():
        decay, root = decay_of(eig_a[...] + eig_c[...] + 0.001)
        rho[...] = decay
        gain[...] = scale / root
        run[...] = carry[0]
        back[count - 1] = decay * carry[1]

        def down(t, _):
            here = count - 2 - t
            back[here] = rho[...] * (z_ref[here + 1] + back[here + 1])
            return 0

        lax.fori_loop(0, count - 1, down, 0)

    run[...] = z_ref[step] + rho[...] * run[...]
    field = gain[...] * (run[...] + back[step])
    lines = table_times(ah[...], al[...], field)
    out_ref[0] = times_table(lines, ch[...], cl[...])


def whole(shape):
    return pl.BlockSpec(shape, lambda t: (0,) * len(shape))


def forward_call(x, tables):
    count, rows, cols = x.shape
    plane = jax.ShapeDtypeStruct((rows, cols), jnp.float32)
    return pl.pallas_call(
        forward_kernel,
        grid=(count,),
        in_specs=[whole(t.shape) for t in tables]
        + [pl.BlockSpec((1, rows, cols), lambda t: (t, 0, 0))],
        out_specs=[
            pl.BlockSpec((1, rows, cols), lambda t: (t, 0, 0)),
            whole((rows, cols)),
            whole((rows, cols)),
        ],
        out_shape=[jax.ShapeDtypeStruct(x.shape, jnp.float32), plane, plane],
        scratch_shapes=[pltpu.VMEM((rows, cols), jnp.float32)] * 2,
    )(*tables, x)


def backward_call(z, carry, tables, scale):
    count, rows, cols = z.shape
    return pl.pallas_call(
        functools.partial(backward_kernel, scale),
        grid=(count,),
        in_specs=[whole(t.shape) for t in tables] + [whole(z.shape), whole(carry.shape)],
        out_specs=pl.BlockSpec((1, rows, cols), lambda t: (t, 0, 0)),
        out_shape=jax.ShapeDtypeStruct(z.shape, jnp.float32),
        scratch_shapes=[pltpu.VMEM((rows, cols), jnp.float32)] * 3
        + [pltpu.VMEM(z.shape, jnp.float32)],
        compiler_params=pltpu.CompilerParams(vmem_limit_bytes=50 * 1024 * 1024),
    )(*tables, z, carry)


def carries(up, down, count, eig_a, eig_c):
    rows, cols = up.shape
    rep_count = lax.axis_size("rep")
    col_count = lax.axis_size("col")
    row_count = lax.axis_size("row")
    group = rep_count * col_count
    part = rows // group
    member = lax.axis_index("rep") * col_count + lax.axis_index("col")
    row = lax.axis_index("row")
    ends = jnp.stack([up, down]).reshape(2, group, part, cols)
    ends = lax.all_to_all(ends, ("rep", "col"), split_axis=1, concat_axis=1)
    eig_part = lax.dynamic_slice_in_dim(jnp.asarray(eig_a), member * part, part, 0)
    rho, _ = decay_of(eig_part[:, None] + jnp.asarray(eig_c)[None, :] + 0.001)
    block = lax.integer_pow(rho, count)
    wide = lax.integer_pow(block, group)
    total_up = ends[0, 0]
    total_down = ends[1, group - 1]
    for j in range(1, group):
        total_up = ends[0, j] + block * total_up
        total_down = ends[1, group - 1 - j] + block * total_down
    every = lax.all_gather(jnp.stack([total_up, total_down]), "row", axis=0)

    def pick(offset, side):
        return lax.dynamic_index_in_dim(every, (row + offset) % row_count, 0, False)[side]

    into_up = pick(0, 0)
    into_down = pick(0, 1)
    for m in range(row_count - 1, 0, -1):
        into_up = pick(row_count - m, 0) + wide * into_up
        into_down = pick(m, 1) + wide * into_down
    closing = 1.0 / (1.0 - lax.integer_pow(wide, row_count))
    ups = [into_up * closing]
    downs = [into_down * closing]
    for j in range(group - 1):
        ups.append(ends[0, j] + block * ups[-1])
        downs.append(ends[1, group - 1 - j] + block * downs[-1])
    back = jnp.stack([jnp.stack(ups), jnp.stack(downs[::-1])])
    back = lax.all_to_all(back, ("rep", "col"), split_axis=1, concat_axis=1)
    return back.reshape(2, rows, cols)


def line_body(sources):
    partial_value = sources[0]
    rep_count = lax.axis_size("rep")
    col_count = lax.axis_size("col")
    slab, width, length_c = partial_value.shape
    length_a = slab * col_count
    length_b = width * lax.axis_size("row")
    half = width // rep_count
    rep = lax.axis_index("rep")
    part = half // col_count
    by_line = partial_value.transpose(1, 0, 2)
    mine = lax.psum_scatter(by_line, "rep", scatter_dimension=0, tiled=True)
    lines = lax.all_to_all(mine, "col", split_axis=0, concat_axis=1, tiled=True)
    high_a, low_a = slab_tables(length_a)
    high_c, low_c = slab_tables(length_c)
    eig_a = eigen_values(length_a)
    eig_c = eigen_values(length_c)
    tables = (
        high_a,
        low_a,
        high_c,
        low_c,
        jnp.asarray(eig_a)[:, None],
        jnp.asarray(eig_c)[None, :],
    )
    modes, up, down = forward_call(lines, tables)
    carry = carries(up, down, part, eig_a, eig_c)
    field = backward_call(modes, carry, tables, 1.0 / (length_a * length_c))
    result = lax.all_to_all(field, ("rep", "col"), split_axis=1, concat_axis=0, tiled=True)
    return result.transpose(1, 0, 2)


def solution(mesh):
    in_specs = (P("rep", "col", "row", None),)
    out_specs = P(("rep", "col"), "row", None)
    ways = mesh.shape["rep"] * mesh.shape["col"]
    split_lines = (NB // mesh.shape["row"]) % ways == 0 and NA % (8 * ways) == 0
    chosen = line_body if split_lines else body
    return jax.shard_map(chosen, mesh=mesh, in_specs=in_specs, out_specs=out_specs, check_vma=False)
```

```python
import functools
import math

import jax
import jax.numpy as jnp
import numpy as np
from jax import lax
from jax.experimental import pallas as pl
from jax.experimental.pallas import tpu as pltpu
from jax.sharding import PartitionSpec as P

NA = 384
NB = 384
NC = 384


highest = lax.Precision.HIGHEST
MESH = pl.DeviceIdType.MESH
GROUP = 8
LANES = 128
VMEM_BYTES = 56 * 1024 * 1024


def wave_tables(freq_index, position, length):
    turns = freq_index[:, None] * position[None, :] % length
    angle = turns.astype(jnp.float32) * (2.0 * math.pi / length)
    return (jnp.cos(angle), jnp.sin(angle))


def matmul_high(first_matrix, second_matrix):
    return jnp.dot(
        first_matrix, second_matrix, precision=highest, preferred_element_type=jnp.float32
    )


def leading_contract(first_matrix, second_matrix):
    return lax.dot_general(
        first_matrix,
        second_matrix,
        (((0,), (0,)), ((), ())),
        precision=highest,
        preferred_element_type=jnp.float32,
    )


def trailing_contract(first_matrix, second_matrix):
    return lax.dot_general(
        first_matrix,
        second_matrix,
        (((1,), (1,)), ((), ())),
        precision=highest,
        preferred_element_type=jnp.float32,
    )


def table_against_rows(table, flat_rows):
    return lax.dot_general(
        table,
        flat_rows,
        (((0,), (1,)), ((), ())),
        precision=highest,
        preferred_element_type=jnp.float32,
    )


def laplace_eigen(wave_index, length):
    sines = jnp.sin(wave_index.astype(jnp.float32) * (math.pi / length))
    return 4.0 * sines * sines


def mirror_modes(values, axis_number):
    return jnp.roll(jnp.flip(values, axis_number), 1, axis_number)


def body(sources):
    partial_value = sources[0]
    density = lax.psum_scatter(partial_value, "rep", scatter_dimension=0, tiled=True)
    slab_rows, line_rows, length_c = density.shape
    rep_count = lax.axis_size("rep")
    col_count = lax.axis_size("col")
    third_len = NC // 2
    freq_block = third_len // (rep_count * col_count)
    half_first = NA // 2
    modes_first = jnp.arange(NA, dtype=jnp.int32)
    modes_second = jnp.arange(NB, dtype=jnp.int32)
    modes_third = jnp.arange(NC, dtype=jnp.int32)
    modes_spec = jnp.arange(third_len, dtype=jnp.int32)
    parity = (1 - 2 * (modes_third % 2)).astype(jnp.float32)
    owner_zero = (lax.axis_index("rep") == 0) & (lax.axis_index("col") == 0)
    flat_density = density.reshape(slab_rows * line_rows, NC)
    cos_spec, sin_spec = wave_tables(modes_spec, modes_third, NC)
    sin_spec = jnp.where(modes_spec[:, None] == 0, -parity[None, :], sin_spec)
    real_third = trailing_contract(flat_density, cos_spec).reshape(slab_rows, line_rows, third_len)
    imag_third = (-trailing_contract(flat_density, sin_spec)).reshape(
        slab_rows, line_rows, third_len
    )
    group_first = modes_first // slab_rows
    first_index = (
        group_first % col_count * (rep_count * slab_rows)
        + group_first // col_count * slab_rows
        + modes_first % slab_rows
    )
    cos_first, sin_first = wave_tables(first_index, modes_first, NA)
    real_in = lax.all_to_all(real_third, ("rep", "col"), split_axis=2, concat_axis=0, tiled=True)
    imag_in = lax.all_to_all(imag_third, ("rep", "col"), split_axis=2, concat_axis=0, tiled=True)
    count = real_in.shape[1]
    flat_real = real_in.reshape(NA, count * freq_block)
    flat_imag = imag_in.reshape(NA, count * freq_block)
    real_out = leading_contract(flat_real, cos_first) + leading_contract(flat_imag, sin_first)
    imag_out = leading_contract(flat_imag, cos_first) - leading_contract(flat_real, sin_first)
    real_first = real_out.reshape(count, freq_block, NA)
    imag_first = imag_out.reshape(count, freq_block, NA)
    packed_r = real_first[:, 0, :]
    packed_i = imag_first[:, 0, :]
    mirror_r = mirror_modes(packed_r, 1)
    mirror_i = mirror_modes(packed_i, 1)
    zero_r = 0.5 * (packed_r + mirror_r)
    zero_i = 0.5 * (packed_i - mirror_i)
    top_r = 0.5 * (packed_i + mirror_i)
    top_i = -0.5 * (packed_r - mirror_r)
    edge_modes = ((modes_first == 0) | (modes_first == half_first))[None, :]
    lower_modes = (modes_first <= half_first)[None, :]
    new_r = jnp.where(lower_modes, zero_r, top_r)
    new_i = jnp.where(edge_modes, top_r, jnp.where(lower_modes, zero_i, top_i))
    real_first = real_first.at[:, 0, :].set(jnp.where(owner_zero, new_r, packed_r))
    imag_first = imag_first.at[:, 0, :].set(jnp.where(owner_zero, new_i, packed_i))
    cos_second, sin_second = wave_tables(modes_second, modes_second, NB)
    real_in = lax.all_to_all(real_first, "row", split_axis=2, concat_axis=0, tiled=True)
    imag_in = lax.all_to_all(imag_first, "row", split_axis=2, concat_axis=0, tiled=True)
    count = real_in.shape[1]
    tail = real_in.shape[2]
    flat_real = real_in.reshape(NB, count * tail)
    flat_imag = imag_in.reshape(NB, count * tail)
    real_out = matmul_high(cos_second, flat_real) + matmul_high(sin_second, flat_imag)
    imag_out = matmul_high(cos_second, flat_imag) - matmul_high(sin_second, flat_real)
    real_second = real_out.reshape(NB, count, tail)
    imag_second = imag_out.reshape(NB, count, tail)
    freq_rows = real_second.shape[2]
    first_freqs = lax.axis_index("row") * freq_rows + jnp.arange(freq_rows, dtype=jnp.int32)
    third_freqs = (
        lax.axis_index("rep") * col_count + lax.axis_index("col")
    ) * freq_block + jnp.arange(freq_block, dtype=jnp.int32)
    scale_all = 1.0 / (NA * NB * NC)
    eigen_second = laplace_eigen(modes_second, NB)
    eigen_first = laplace_eigen(first_freqs, NA)
    total = (
        eigen_second[:, None, None]
        + laplace_eigen(third_freqs, NC)[None, :, None]
        + eigen_first[None, None, :]
        + 0.001
    )
    green = 1.0 / total * scale_all
    filt_real = real_second * green
    filt_imag = imag_second * green
    wave_r = real_second[:, 0, :]
    wave_i = imag_second[:, 0, :]
    green_zero = green[:, 0, :]
    green_top = 1.0 / (eigen_second[:, None] + 4.0 + eigen_first[None, :] + 0.001) * scale_all
    mean_green = 0.5 * (green_zero + green_top)
    diff_green = 0.5 * (green_zero - green_top)
    mixed_r = mean_green * wave_r + diff_green * mirror_modes(wave_r, 0)
    mixed_i = mean_green * wave_i - diff_green * mirror_modes(wave_i, 0)
    lower_freqs = ((first_freqs > 0) & (first_freqs < half_first))[None, :]
    upper_freqs = (first_freqs > half_first)[None, :]
    slot_r = jnp.where(
        lower_freqs, green_zero * wave_r, jnp.where(upper_freqs, green_top * wave_r, mixed_r)
    )
    slot_i = jnp.where(
        lower_freqs, green_zero * wave_i, jnp.where(upper_freqs, green_top * wave_i, mixed_i)
    )
    filt_real = filt_real.at[:, 0, :].set(jnp.where(owner_zero, slot_r, filt_real[:, 0, :]))
    filt_imag = filt_imag.at[:, 0, :].set(jnp.where(owner_zero, slot_i, filt_imag[:, 0, :]))
    flat_real = filt_real.reshape(NB, freq_block * freq_rows)
    flat_imag = filt_imag.reshape(NB, freq_block * freq_rows)
    real_back = (matmul_high(cos_second, flat_real) - matmul_high(sin_second, flat_imag)).reshape(
        NB, freq_block, freq_rows
    )
    imag_back = (matmul_high(cos_second, flat_imag) + matmul_high(sin_second, flat_real)).reshape(
        NB, freq_block, freq_rows
    )
    cos_inverse, sin_inverse = wave_tables(modes_first, modes_first, NA)
    real_in = lax.all_to_all(real_back, "row", split_axis=0, concat_axis=2, tiled=True)
    imag_in = lax.all_to_all(imag_back, "row", split_axis=0, concat_axis=2, tiled=True)
    b_count = real_in.shape[0]
    count = real_in.shape[1]
    flat_real_in = real_in.reshape(b_count * count, NA)
    flat_imag_in = imag_in.reshape(b_count * count, NA)
    real_out = table_against_rows(cos_inverse, flat_real_in) - table_against_rows(
        sin_inverse, flat_imag_in
    )
    imag_out = table_against_rows(cos_inverse, flat_imag_in) + table_against_rows(
        sin_inverse, flat_real_in
    )
    real_lines = real_out.reshape(NA, b_count, count)
    imag_lines = imag_out.reshape(NA, b_count, count)
    field_r = real_lines[:, :, 0]
    field_i = imag_lines[:, :, 0]
    spec_r = (matmul_high(cos_inverse, field_r) + matmul_high(sin_inverse, field_i)) * (1.0 / NA)
    spec_i = (matmul_high(cos_inverse, field_i) - matmul_high(sin_inverse, field_r)) * (1.0 / NA)
    mirror_r = mirror_modes(spec_r, 0)
    mirror_i = mirror_modes(spec_i, 0)
    lower_lines = ((modes_first > 0) & (modes_first < half_first))[:, None]
    upper_lines = (modes_first > half_first)[:, None]
    joined_r = jnp.where(
        lower_lines, spec_r + mirror_i, jnp.where(upper_lines, mirror_r - spec_i, spec_r)
    )
    joined_i = jnp.where(
        lower_lines, spec_i + mirror_r, jnp.where(upper_lines, spec_r - mirror_i, spec_i)
    )
    rebuilt_r = matmul_high(cos_inverse, joined_r) - matmul_high(sin_inverse, joined_i)
    rebuilt_i = matmul_high(cos_inverse, joined_i) + matmul_high(sin_inverse, joined_r)
    real_lines = real_lines.at[:, :, 0].set(jnp.where(owner_zero, rebuilt_r, field_r))
    imag_lines = imag_lines.at[:, :, 0].set(jnp.where(owner_zero, rebuilt_i, field_i))
    cos_final, sin_final = wave_tables(modes_spec, modes_third, NC)
    weight = jnp.where(modes_spec == 0, 1.0, 2.0).astype(jnp.float32)[:, None]
    cos_final = weight * cos_final
    sin_final = jnp.where(modes_spec[:, None] == 0, -parity[None, :], 2.0 * sin_final)
    real_in = lax.all_to_all(real_lines, ("rep", "col"), split_axis=0, concat_axis=2, tiled=True)
    imag_in = lax.all_to_all(imag_lines, ("rep", "col"), split_axis=0, concat_axis=2, tiled=True)
    a_count = real_in.shape[0]
    count = real_in.shape[1]
    spec_len = real_in.shape[2]
    flat_real_in = real_in.reshape(a_count * count, spec_len)
    flat_imag_in = imag_in.reshape(a_count * count, spec_len)
    result = matmul_high(flat_real_in, cos_final) - matmul_high(flat_imag_in, sin_final)
    return result.reshape(a_count, count, NC)


def slab_tables(length):
    turns = np.outer(np.arange(length), np.arange(length)) % length
    angle = turns * (2.0 * np.pi / length)
    table = np.cos(angle) + np.sin(angle)
    high = table.astype(jnp.bfloat16)
    low = (table - high.astype(np.float64)).astype(jnp.bfloat16)
    return jnp.asarray(high), jnp.asarray(low)


def eigen_values(length):
    sines = np.sin(np.arange(length) * (np.pi / length))
    return (4.0 * sines * sines).astype(np.float32)


def halves(value):
    high = value.astype(jnp.bfloat16)
    low = (value - high.astype(jnp.float32)).astype(jnp.bfloat16)
    return high, low


def dot_f32(left, right):
    return jnp.dot(left, right, preferred_element_type=jnp.float32)


def times_table(value, high, low):
    top, rest = halves(value)
    return dot_f32(top, high) + dot_f32(top, low) + dot_f32(rest, high)


def table_times(high, low, value):
    top, rest = halves(value)
    return dot_f32(high, top) + dot_f32(low, top) + dot_f32(high, rest)


def decay_of(shift):
    root = jnp.sqrt(shift * (shift + 4.0))
    return 2.0 / (2.0 + shift + root), root


def peer_signal(semaphore, rep, col):
    pl.semaphore_signal(
        semaphore, inc=1, device_id={"rep": rep, "col": col}, device_id_type=MESH
    )


def send(source, target, send_sem, recv_sem, rep, col):
    return pltpu.make_async_remote_copy(
        src_ref=source,
        dst_ref=target,
        send_sem=send_sem,
        recv_sem=recv_sem,
        device_id={"rep": rep, "col": col},
        device_id_type=MESH,
    )


def forward_kernel(
    ah, al, ch, cl, eig_a, eig_c, x_ref,
    z_ref, up_ref, down_ref,
    own, other, sums, far, lines, rho, power,
    own_sem, rep_send, rep_recv, col_send, col_recv,
):
    rep = lax.axis_index("rep")
    col = lax.axis_index("col")
    groups, bands, tall, band = own.shape
    slab = tall // GROUP
    count = z_ref.shape[0]
    half = groups * GROUP

    barrier = pltpu.get_barrier_semaphore()
    peer_signal(barrier, 1 - rep, col)
    peer_signal(barrier, rep, 1 - col)
    pl.semaphore_wait(barrier, 2)

    def place(n):
        return (n + 1 - col) % groups

    def rep_copy(n, j):
        start = pl.multiple_of((1 - rep) * half + place(n) * GROUP, GROUP)
        return send(
            x_ref.at[:, pl.ds(start, GROUP), pl.ds(j * band, band)],
            other.at[place(n), j].reshape(slab, GROUP, band),
            rep_send.at[n, j],
            rep_recv.at[n, j],
            1 - rep,
            col,
        )

    def own_copy(n, j):
        start = pl.multiple_of(rep * half + place(n) * GROUP, GROUP)
        return pltpu.make_async_copy(
            x_ref.at[:, pl.ds(start, GROUP), pl.ds(j * band, band)],
            own.at[place(n), j].reshape(slab, GROUP, band),
            own_sem.at[n, j],
        )

    def col_copy(t):
        return send(
            sums.at[(1 - col) * count + t],
            far.at[t],
            col_send.at[t],
            col_recv.at[t],
            rep,
            1 - col,
        )

    for n in range(groups):
        for j in range(bands):
            rep_copy(n, j).start()
            own_copy(n, j).start()
    decay, _ = decay_of(eig_a[...] + eig_c[...] + 0.001)
    rho[...] = decay
    power[...] = jnp.ones_like(decay)
    up_ref[...] = jnp.zeros_like(decay)
    down_ref[...] = jnp.zeros_like(decay)

    for n in range(groups):
        for j in range(bands):
            rep_copy(n, j).wait_recv()
            own_copy(n, j).wait()

        def add(s, _):
            line = place(n) * GROUP + s
            rows = pl.ds(s, slab, stride=GROUP)
            for j in range(bands):
                sums[line, :, j * band : (j + 1) * band] = (
                    own[place(n), j, rows, :] + other[place(n), j, rows, :]
                )
            t = line - (1 - col) * count

            @pl.when((t >= 0) & (t < count))
            def _():
                col_copy(t).start()

            return 0

        lax.fori_loop(0, GROUP, add, 0)

    def transform(t, _):
        here = pl.ds(pl.multiple_of(col * slab, 8), slab)
        there = pl.ds(pl.multiple_of((1 - col) * slab, 8), slab)
        lines[here, :] = times_table(sums[col * count + t], ch[...], cl[...])
        col_copy(t).wait_recv()
        lines[there, :] = times_table(far[t], ch[...], cl[...])
        modes = table_times(ah[...], al[...], lines[...])
        z_ref[t] = modes
        up_ref[...] = modes + rho[...] * up_ref[...]
        down_ref[...] = down_ref[...] + power[...] * modes
        power[...] = power[...] * rho[...]
        return 0

    lax.fori_loop(0, count, transform, 0)
    for n in range(groups):
        for j in range(bands):
            rep_copy(n, j).wait_send()

    def drain(t, _):
        col_copy(t).wait_send()
        return 0

    lax.fori_loop(0, count, drain, 0)


def backward_kernel(
    scale,
    ah, al, ch, cl, eig_a, eig_c, z_ref, carry,
    out_ref,
    rho, gain, run, back, planes,
    own_sem, send_sem, recv_sem,
):
    rep = lax.axis_index("rep")
    col = lax.axis_index("col")
    count = z_ref.shape[0]
    slab = out_ref.shape[1]
    offsets = ((0, 1), (1, 1), (1, 0))

    barrier = pltpu.get_barrier_semaphore()
    for flip_rep, flip_col in offsets:
        peer_signal(barrier, (rep + flip_rep) % 2, (col + flip_col) % 2)
    pl.semaphore_wait(barrier, 3)

    mine = rep * 2 + col

    def peer_copy(k, t):
        to_rep = (rep + offsets[k][0]) % 2
        to_col = (col + offsets[k][1]) % 2
        start = pl.multiple_of((to_rep * 2 + to_col) * slab, 8)
        return send(
            planes.at[t, pl.ds(start, slab), :],
            out_ref.at[mine * count + t],
            send_sem.at[k, t],
            recv_sem.at[k, t],
            to_rep,
            to_col,
        )

    def own_copy(t):
        start = pl.multiple_of(mine * slab, 8)
        return pltpu.make_async_copy(
            planes.at[t, pl.ds(start, slab), :], out_ref.at[mine * count + t], own_sem.at[t]
        )

    decay, root = decay_of(eig_a[...] + eig_c[...] + 0.001)
    rho[...] = decay
    gain[...] = scale / root
    run[...] = carry[0]
    back[count - 1] = decay * carry[1]

    def down(t, _):
        here = count - 2 - t
        back[here] = rho[...] * (z_ref[here + 1] + back[here + 1])
        return 0

    lax.fori_loop(0, count - 1, down, 0)

    def emit(t, _):
        run[...] = z_ref[t] + rho[...] * run[...]
        field = gain[...] * (run[...] + back[t])
        lines = table_times(ah[...], al[...], field)
        planes[t] = times_table(lines, ch[...], cl[...])
        for k in range(3):
            peer_copy(k, t).start()
        own_copy(t).start()
        return 0

    lax.fori_loop(0, count, emit, 0)

    def drain(t, _):
        own_copy(t).wait()
        for k in range(3):
            peer_copy(k, t).wait()
        return 0

    lax.fori_loop(0, count, drain, 0)


def forward_call(x, tables):
    slab, width, cols = x.shape
    rows = slab * 2
    half = width // 2
    count = half // 2
    plane = jax.ShapeDtypeStruct((rows, cols), jnp.float32)
    modes = jax.ShapeDtypeStruct((count, rows, cols), jnp.float32)
    vmem = pl.BlockSpec(memory_space=pltpu.VMEM)
    groups = half // GROUP
    dma = pltpu.SemaphoreType.DMA
    f32 = jnp.float32
    return pl.pallas_call(
        forward_kernel,
        in_specs=[vmem] * len(tables) + [pl.BlockSpec(memory_space=pl.ANY)],
        out_specs=[vmem] * 3,
        out_shape=[modes, plane, plane],
        scratch_shapes=[
            pltpu.VMEM((groups, cols // LANES, slab * GROUP, LANES), f32),
            pltpu.VMEM((groups, cols // LANES, slab * GROUP, LANES), f32),
            pltpu.VMEM((half, slab, cols), f32),
            pltpu.VMEM((count, slab, cols), f32),
            pltpu.VMEM((rows, cols), f32),
            pltpu.VMEM((rows, cols), f32),
            pltpu.VMEM((rows, cols), f32),
            dma((groups, cols // LANES)),
            dma((groups, cols // LANES)),
            dma((groups, cols // LANES)),
            dma((count,)),
            dma((count,)),
        ],
        compiler_params=pltpu.CompilerParams(
            collective_id=0, has_side_effects=True, vmem_limit_bytes=VMEM_BYTES
        ),
    )(*tables, x)


def backward_call(z, carry, tables, scale):
    count, rows, cols = z.shape
    vmem = pl.BlockSpec(memory_space=pltpu.VMEM)
    dma = pltpu.SemaphoreType.DMA
    return pl.pallas_call(
        functools.partial(backward_kernel, scale),
        in_specs=[vmem] * (len(tables) + 2),
        out_specs=pl.BlockSpec(memory_space=pl.ANY),
        out_shape=jax.ShapeDtypeStruct((count * 4, rows // 4, cols), jnp.float32),
        scratch_shapes=[pltpu.VMEM((rows, cols), jnp.float32)] * 3
        + [pltpu.VMEM(z.shape, jnp.float32)] * 2
        + [dma((count,)), dma((3, count)), dma((3, count))],
        compiler_params=pltpu.CompilerParams(
            collective_id=1, has_side_effects=True, vmem_limit_bytes=VMEM_BYTES
        ),
    )(*tables, z, carry)


def carries(up, down, count, eig_a, eig_c):
    rows, cols = up.shape
    rep_count = lax.axis_size("rep")
    col_count = lax.axis_size("col")
    row_count = lax.axis_size("row")
    group = rep_count * col_count
    part = rows // group
    member = lax.axis_index("rep") * col_count + lax.axis_index("col")
    row = lax.axis_index("row")
    ends = jnp.stack([up, down]).reshape(2, group, part, cols)
    ends = lax.all_to_all(ends, ("rep", "col"), split_axis=1, concat_axis=1)
    eig_part = lax.dynamic_slice_in_dim(jnp.asarray(eig_a), member * part, part, 0)
    rho, _ = decay_of(eig_part[:, None] + jnp.asarray(eig_c)[None, :] + 0.001)
    block = lax.integer_pow(rho, count)
    wide = lax.integer_pow(block, group)
    total_up = ends[0, 0]
    total_down = ends[1, group - 1]
    for j in range(1, group):
        total_up = ends[0, j] + block * total_up
        total_down = ends[1, group - 1 - j] + block * total_down
    every = lax.all_gather(jnp.stack([total_up, total_down]), "row", axis=0)

    def pick(offset, side):
        return lax.dynamic_index_in_dim(every, (row + offset) % row_count, 0, False)[side]

    into_up = pick(0, 0)
    into_down = pick(0, 1)
    for m in range(row_count - 1, 0, -1):
        into_up = pick(row_count - m, 0) + wide * into_up
        into_down = pick(m, 1) + wide * into_down
    closing = 1.0 / (1.0 - lax.integer_pow(wide, row_count))
    ups = [into_up * closing]
    downs = [into_down * closing]
    for j in range(group - 1):
        ups.append(ends[0, j] + block * ups[-1])
        downs.append(ends[1, group - 1 - j] + block * downs[-1])
    back = jnp.stack([jnp.stack(ups), jnp.stack(downs[::-1])])
    back = lax.all_to_all(back, ("rep", "col"), split_axis=1, concat_axis=1)
    return back.reshape(2, rows, cols)


def line_body(sources):
    partial_value = sources[0]
    slab, width, length_c = partial_value.shape
    length_a = slab * lax.axis_size("col")
    high_a, low_a = slab_tables(length_a)
    high_c, low_c = slab_tables(length_c)
    eig_a = eigen_values(length_a)
    eig_c = eigen_values(length_c)
    tables = (
        high_a,
        low_a,
        high_c,
        low_c,
        jnp.asarray(eig_a)[:, None],
        jnp.asarray(eig_c)[None, :],
    )
    modes, up, down = forward_call(partial_value, tables)
    carry = carries(up, down, modes.shape[0], eig_a, eig_c)
    result = backward_call(modes, carry, tables, 1.0 / (length_a * length_c))
    return result.transpose(1, 0, 2)


def solution(mesh):
    in_specs = (P("rep", "col", "row", None),)
    out_specs = P(("rep", "col"), "row", None)
    pairs = mesh.shape["rep"] == 2 and mesh.shape["col"] == 2
    split_lines = pairs and (NB // mesh.shape["row"]) % (2 * GROUP) == 0 and NA % 32 == 0 and NC % LANES == 0
    chosen = line_body if split_lines else body
    return jax.shard_map(chosen, mesh=mesh, in_specs=in_specs, out_specs=out_specs, check_vma=False)
```

```python
import functools
import math

import jax
import jax.numpy as jnp
import numpy as np
from jax import lax
from jax.experimental import pallas as pl
from jax.experimental.pallas import tpu as pltpu
from jax.sharding import PartitionSpec as P

NA = 384
NB = 384
NC = 384


highest = lax.Precision.HIGHEST
MESH = pl.DeviceIdType.MESH
GROUP = 8
LANES = 128
VMEM_BYTES = 56 * 1024 * 1024


def wave_tables(freq_index, position, length):
    turns = freq_index[:, None] * position[None, :] % length
    angle = turns.astype(jnp.float32) * (2.0 * math.pi / length)
    return (jnp.cos(angle), jnp.sin(angle))


def matmul_high(first_matrix, second_matrix):
    return jnp.dot(
        first_matrix, second_matrix, precision=highest, preferred_element_type=jnp.float32
    )


def leading_contract(first_matrix, second_matrix):
    return lax.dot_general(
        first_matrix,
        second_matrix,
        (((0,), (0,)), ((), ())),
        precision=highest,
        preferred_element_type=jnp.float32,
    )


def trailing_contract(first_matrix, second_matrix):
    return lax.dot_general(
        first_matrix,
        second_matrix,
        (((1,), (1,)), ((), ())),
        precision=highest,
        preferred_element_type=jnp.float32,
    )


def table_against_rows(table, flat_rows):
    return lax.dot_general(
        table,
        flat_rows,
        (((0,), (1,)), ((), ())),
        precision=highest,
        preferred_element_type=jnp.float32,
    )


def laplace_eigen(wave_index, length):
    sines = jnp.sin(wave_index.astype(jnp.float32) * (math.pi / length))
    return 4.0 * sines * sines


def mirror_modes(values, axis_number):
    return jnp.roll(jnp.flip(values, axis_number), 1, axis_number)


def body(sources):
    partial_value = sources[0]
    density = lax.psum_scatter(partial_value, "rep", scatter_dimension=0, tiled=True)
    slab_rows, line_rows, length_c = density.shape
    rep_count = lax.axis_size("rep")
    col_count = lax.axis_size("col")
    third_len = NC // 2
    freq_block = third_len // (rep_count * col_count)
    half_first = NA // 2
    modes_first = jnp.arange(NA, dtype=jnp.int32)
    modes_second = jnp.arange(NB, dtype=jnp.int32)
    modes_third = jnp.arange(NC, dtype=jnp.int32)
    modes_spec = jnp.arange(third_len, dtype=jnp.int32)
    parity = (1 - 2 * (modes_third % 2)).astype(jnp.float32)
    owner_zero = (lax.axis_index("rep") == 0) & (lax.axis_index("col") == 0)
    flat_density = density.reshape(slab_rows * line_rows, NC)
    cos_spec, sin_spec = wave_tables(modes_spec, modes_third, NC)
    sin_spec = jnp.where(modes_spec[:, None] == 0, -parity[None, :], sin_spec)
    real_third = trailing_contract(flat_density, cos_spec).reshape(slab_rows, line_rows, third_len)
    imag_third = (-trailing_contract(flat_density, sin_spec)).reshape(
        slab_rows, line_rows, third_len
    )
    group_first = modes_first // slab_rows
    first_index = (
        group_first % col_count * (rep_count * slab_rows)
        + group_first // col_count * slab_rows
        + modes_first % slab_rows
    )
    cos_first, sin_first = wave_tables(first_index, modes_first, NA)
    real_in = lax.all_to_all(real_third, ("rep", "col"), split_axis=2, concat_axis=0, tiled=True)
    imag_in = lax.all_to_all(imag_third, ("rep", "col"), split_axis=2, concat_axis=0, tiled=True)
    count = real_in.shape[1]
    flat_real = real_in.reshape(NA, count * freq_block)
    flat_imag = imag_in.reshape(NA, count * freq_block)
    real_out = leading_contract(flat_real, cos_first) + leading_contract(flat_imag, sin_first)
    imag_out = leading_contract(flat_imag, cos_first) - leading_contract(flat_real, sin_first)
    real_first = real_out.reshape(count, freq_block, NA)
    imag_first = imag_out.reshape(count, freq_block, NA)
    packed_r = real_first[:, 0, :]
    packed_i = imag_first[:, 0, :]
    mirror_r = mirror_modes(packed_r, 1)
    mirror_i = mirror_modes(packed_i, 1)
    zero_r = 0.5 * (packed_r + mirror_r)
    zero_i = 0.5 * (packed_i - mirror_i)
    top_r = 0.5 * (packed_i + mirror_i)
    top_i = -0.5 * (packed_r - mirror_r)
    edge_modes = ((modes_first == 0) | (modes_first == half_first))[None, :]
    lower_modes = (modes_first <= half_first)[None, :]
    new_r = jnp.where(lower_modes, zero_r, top_r)
    new_i = jnp.where(edge_modes, top_r, jnp.where(lower_modes, zero_i, top_i))
    real_first = real_first.at[:, 0, :].set(jnp.where(owner_zero, new_r, packed_r))
    imag_first = imag_first.at[:, 0, :].set(jnp.where(owner_zero, new_i, packed_i))
    cos_second, sin_second = wave_tables(modes_second, modes_second, NB)
    real_in = lax.all_to_all(real_first, "row", split_axis=2, concat_axis=0, tiled=True)
    imag_in = lax.all_to_all(imag_first, "row", split_axis=2, concat_axis=0, tiled=True)
    count = real_in.shape[1]
    tail = real_in.shape[2]
    flat_real = real_in.reshape(NB, count * tail)
    flat_imag = imag_in.reshape(NB, count * tail)
    real_out = matmul_high(cos_second, flat_real) + matmul_high(sin_second, flat_imag)
    imag_out = matmul_high(cos_second, flat_imag) - matmul_high(sin_second, flat_real)
    real_second = real_out.reshape(NB, count, tail)
    imag_second = imag_out.reshape(NB, count, tail)
    freq_rows = real_second.shape[2]
    first_freqs = lax.axis_index("row") * freq_rows + jnp.arange(freq_rows, dtype=jnp.int32)
    third_freqs = (
        lax.axis_index("rep") * col_count + lax.axis_index("col")
    ) * freq_block + jnp.arange(freq_block, dtype=jnp.int32)
    scale_all = 1.0 / (NA * NB * NC)
    eigen_second = laplace_eigen(modes_second, NB)
    eigen_first = laplace_eigen(first_freqs, NA)
    total = (
        eigen_second[:, None, None]
        + laplace_eigen(third_freqs, NC)[None, :, None]
        + eigen_first[None, None, :]
        + 0.001
    )
    green = 1.0 / total * scale_all
    filt_real = real_second * green
    filt_imag = imag_second * green
    wave_r = real_second[:, 0, :]
    wave_i = imag_second[:, 0, :]
    green_zero = green[:, 0, :]
    green_top = 1.0 / (eigen_second[:, None] + 4.0 + eigen_first[None, :] + 0.001) * scale_all
    mean_green = 0.5 * (green_zero + green_top)
    diff_green = 0.5 * (green_zero - green_top)
    mixed_r = mean_green * wave_r + diff_green * mirror_modes(wave_r, 0)
    mixed_i = mean_green * wave_i - diff_green * mirror_modes(wave_i, 0)
    lower_freqs = ((first_freqs > 0) & (first_freqs < half_first))[None, :]
    upper_freqs = (first_freqs > half_first)[None, :]
    slot_r = jnp.where(
        lower_freqs, green_zero * wave_r, jnp.where(upper_freqs, green_top * wave_r, mixed_r)
    )
    slot_i = jnp.where(
        lower_freqs, green_zero * wave_i, jnp.where(upper_freqs, green_top * wave_i, mixed_i)
    )
    filt_real = filt_real.at[:, 0, :].set(jnp.where(owner_zero, slot_r, filt_real[:, 0, :]))
    filt_imag = filt_imag.at[:, 0, :].set(jnp.where(owner_zero, slot_i, filt_imag[:, 0, :]))
    flat_real = filt_real.reshape(NB, freq_block * freq_rows)
    flat_imag = filt_imag.reshape(NB, freq_block * freq_rows)
    real_back = (matmul_high(cos_second, flat_real) - matmul_high(sin_second, flat_imag)).reshape(
        NB, freq_block, freq_rows
    )
    imag_back = (matmul_high(cos_second, flat_imag) + matmul_high(sin_second, flat_real)).reshape(
        NB, freq_block, freq_rows
    )
    cos_inverse, sin_inverse = wave_tables(modes_first, modes_first, NA)
    real_in = lax.all_to_all(real_back, "row", split_axis=0, concat_axis=2, tiled=True)
    imag_in = lax.all_to_all(imag_back, "row", split_axis=0, concat_axis=2, tiled=True)
    b_count = real_in.shape[0]
    count = real_in.shape[1]
    flat_real_in = real_in.reshape(b_count * count, NA)
    flat_imag_in = imag_in.reshape(b_count * count, NA)
    real_out = table_against_rows(cos_inverse, flat_real_in) - table_against_rows(
        sin_inverse, flat_imag_in
    )
    imag_out = table_against_rows(cos_inverse, flat_imag_in) + table_against_rows(
        sin_inverse, flat_real_in
    )
    real_lines = real_out.reshape(NA, b_count, count)
    imag_lines = imag_out.reshape(NA, b_count, count)
    field_r = real_lines[:, :, 0]
    field_i = imag_lines[:, :, 0]
    spec_r = (matmul_high(cos_inverse, field_r) + matmul_high(sin_inverse, field_i)) * (1.0 / NA)
    spec_i = (matmul_high(cos_inverse, field_i) - matmul_high(sin_inverse, field_r)) * (1.0 / NA)
    mirror_r = mirror_modes(spec_r, 0)
    mirror_i = mirror_modes(spec_i, 0)
    lower_lines = ((modes_first > 0) & (modes_first < half_first))[:, None]
    upper_lines = (modes_first > half_first)[:, None]
    joined_r = jnp.where(
        lower_lines, spec_r + mirror_i, jnp.where(upper_lines, mirror_r - spec_i, spec_r)
    )
    joined_i = jnp.where(
        lower_lines, spec_i + mirror_r, jnp.where(upper_lines, spec_r - mirror_i, spec_i)
    )
    rebuilt_r = matmul_high(cos_inverse, joined_r) - matmul_high(sin_inverse, joined_i)
    rebuilt_i = matmul_high(cos_inverse, joined_i) + matmul_high(sin_inverse, joined_r)
    real_lines = real_lines.at[:, :, 0].set(jnp.where(owner_zero, rebuilt_r, field_r))
    imag_lines = imag_lines.at[:, :, 0].set(jnp.where(owner_zero, rebuilt_i, field_i))
    cos_final, sin_final = wave_tables(modes_spec, modes_third, NC)
    weight = jnp.where(modes_spec == 0, 1.0, 2.0).astype(jnp.float32)[:, None]
    cos_final = weight * cos_final
    sin_final = jnp.where(modes_spec[:, None] == 0, -parity[None, :], 2.0 * sin_final)
    real_in = lax.all_to_all(real_lines, ("rep", "col"), split_axis=0, concat_axis=2, tiled=True)
    imag_in = lax.all_to_all(imag_lines, ("rep", "col"), split_axis=0, concat_axis=2, tiled=True)
    a_count = real_in.shape[0]
    count = real_in.shape[1]
    spec_len = real_in.shape[2]
    flat_real_in = real_in.reshape(a_count * count, spec_len)
    flat_imag_in = imag_in.reshape(a_count * count, spec_len)
    result = matmul_high(flat_real_in, cos_final) - matmul_high(flat_imag_in, sin_final)
    return result.reshape(a_count, count, NC)


def slab_tables(length):
    turns = np.outer(np.arange(length), np.arange(length)) % length
    angle = turns * (2.0 * np.pi / length)
    table = np.cos(angle) + np.sin(angle)
    high = table.astype(jnp.bfloat16)
    low = (table - high.astype(np.float64)).astype(jnp.bfloat16)
    return jnp.asarray(high), jnp.asarray(low)


def eigen_values(length):
    sines = np.sin(np.arange(length) * (np.pi / length))
    return (4.0 * sines * sines).astype(np.float32)


def halves(value):
    high = value.astype(jnp.bfloat16)
    low = (value - high.astype(jnp.float32)).astype(jnp.bfloat16)
    return high, low


def dot_f32(left, right):
    return jnp.dot(left, right, preferred_element_type=jnp.float32)


def times_table(value, high, low):
    top, rest = halves(value)
    return dot_f32(top, high) + dot_f32(top, low) + dot_f32(rest, high)


def table_times(high, low, value):
    top, rest = halves(value)
    return dot_f32(high, top) + dot_f32(low, top) + dot_f32(high, rest)


def decay_of(shift):
    root = jnp.sqrt(shift * (shift + 4.0))
    return 2.0 / (2.0 + shift + root), root


def peer_signal(semaphore, device):
    pl.semaphore_signal(semaphore, inc=1, device_id=device, device_id_type=MESH)


def send(source, target, send_sem, recv_sem, device):
    return pltpu.make_async_remote_copy(
        src_ref=source,
        dst_ref=target,
        send_sem=send_sem,
        recv_sem=recv_sem,
        device_id=device,
        device_id_type=MESH,
    )


def power_of(base, exponent):
    result = None
    while exponent:
        if exponent & 1:
            result = base if result is None else result * base
        base = base * base
        exponent >>= 1
    return result


def exchange_carries(
    depths, count, up_ref, down_ref, rho, carry,
    e_in, f_out, f_in, g_out, g_in, h_out, h_in, c_out, c_in, x_out, x_in, y_in, r_out,
    sends, recvs,
):
    rep = lax.axis_index("rep")
    col = lax.axis_index("col")
    row = lax.axis_index("row")
    x = row % 2
    z = row // 2
    depth = depths
    tall = depth * 8
    chunk = tall * 4
    chunks = up_ref.shape[0] // chunk
    other_rep = {"rep": 1 - rep}
    other_col = {"col": 1 - col}
    other_x = {"row": z * 2 + 1 - x}
    ends = (up_ref, down_ref)

    def at_z(m):
        return (z + m) % depth

    def rows_of(q):
        return pl.multiple_of(q * chunk + rep * (2 * tall), 8)

    def theta(start, size, blocks):
        return power_of(rho[pl.ds(start, size), :], count * blocks)

    def copy(source, target, q, n, device):
        return send(source, target, sends.at[q, n], recvs.at[q, n], device)

    def rep_in(q):
        start = pl.multiple_of(q * chunk + (1 - rep) * (2 * tall), 8)
        return [
            copy(ends[k].at[pl.ds(start, 2 * tall), :], e_in.at[q, k], q, k, other_rep)
            for k in range(2)
        ]

    def col_in(q):
        return [copy(f_out.at[q, col], f_in.at[q], q, 2, other_col)]

    def x_send(q):
        start = pl.multiple_of((1 - x) * tall, 8)
        return [copy(g_out.at[q, pl.ds(start, tall), :], g_in.at[q], q, 3, other_x)]

    def z_send(q):
        return [
            copy(
                h_out.at[q, pl.ds(pl.multiple_of(at_z(m) * 8, 8), 8), :],
                h_in.at[q, z],
                q,
                3 + m,
                {"row": at_z(m) * 2 + x},
            )
            for m in range(1, depth)
        ]

    def z_back(q):
        return [
            copy(
                c_out.at[q, at_z(m)],
                c_in.at[q, pl.ds(pl.multiple_of(z * 8, 8), 8), :],
                q,
                2 + depth + m,
                {"row": at_z(m) * 2 + x},
            )
            for m in range(1, depth)
        ]

    def x_back(q):
        here = pl.ds(pl.multiple_of(x * tall, 8), tall)
        return [copy(x_out.at[q], x_in.at[q, here, :], q, 2 + 2 * depth, other_x)]

    def col_back(q):
        return [copy(x_in.at[q], y_in.at[q], q, 3 + 2 * depth, other_col)]

    def rep_back(q):
        return [
            copy(
                r_out.at[q, k],
                carry.at[k, pl.ds(rows_of(q), 2 * tall), :],
                q,
                4 + 2 * depth + k,
                other_rep,
            )
            for k in range(2)
        ]

    def ends_of(q, k):
        mine = ends[k][pl.ds(rows_of(q), 2 * tall), :]
        theirs = e_in[q, k]
        first = jnp.where(rep == 0, mine, theirs)
        second = jnp.where(rep == 0, theirs, mine)
        return first, second

    def join_rep(q):
        block = theta(rows_of(q), 2 * tall, 1)
        first, second = ends_of(q, 0)
        f_out[q, 0] = second + block * first
        first, second = ends_of(q, 1)
        f_out[q, 1] = first + block * second

    def join_col(q):
        g_out[q] = f_out[q, 1 - col] + theta(rows_of(q), 2 * tall, 2) * f_in[q]

    def quarter(q):
        return pl.multiple_of(rows_of(q) + x * tall, 8)

    def mine_x(q):
        return g_out[q, pl.ds(pl.multiple_of(x * tall, 8), tall), :]

    def join_x(q):
        near = jnp.where(x == col, mine_x(q), g_in[q])
        away = jnp.where(x == col, g_in[q], mine_x(q))
        h_out[q] = near + theta(quarter(q), tall, 4) * away
        h_in[q, z] = h_out[q, pl.ds(pl.multiple_of(z * 8, 8), 8), :]

    def join_z(q):
        wide = theta(pl.multiple_of(quarter(q) + z * 8, 8), 8, 8)
        closing = 1.0 / (1.0 - power_of(wide, depth))
        step = 2 * col - 1
        for target in range(depth):
            total = h_in[q, target]
            for m in range(depth - 1, 0, -1):
                total = h_in[q, (target + depth - step * m) % depth] + wide * total
            c_out[q, target] = total * closing
        c_in[q, pl.ds(pl.multiple_of(z * 8, 8), 8), :] = c_out[q, z]

    def split_x(q):
        into = c_in[q]
        away = jnp.where(x == col, g_in[q], mine_x(q))
        later = away + theta(quarter(q), tall, 4) * into
        x_in[q, pl.ds(pl.multiple_of(x * tall, 8), tall), :] = jnp.where(x == col, later, into)
        x_out[q] = jnp.where(x == col, into, later)

    def split_rep(q):
        start = rows_of(q)
        here = pl.ds(start, 2 * tall)
        block = theta(start, 2 * tall, 1)
        handled = f_in[q] + theta(start, 2 * tall, 2) * x_in[q]
        into_up = jnp.where(col == 1, handled, y_in[q])
        into_down = jnp.where(col == 1, y_in[q], handled)
        later_up = ends_of(q, 0)[0] + block * into_up
        later_down = ends_of(q, 1)[1] + block * into_down
        carry[0, here, :] = jnp.where(rep == 0, into_up, later_up)
        carry[1, here, :] = jnp.where(rep == 0, later_down, into_down)
        r_out[q, 0] = jnp.where(rep == 0, later_up, into_up)
        r_out[q, 1] = jnp.where(rep == 0, into_down, later_down)

    def nothing(q):
        return None

    moves = (rep_in, col_in, x_send, z_send, z_back, x_back, col_back, rep_back)
    works = (nothing, join_rep, join_col, join_x, join_z, split_x, nothing, split_rep, nothing)
    for moment in range(chunks + len(moves)):
        for q in range(chunks):
            phase = moment - q
            if phase < 0 or phase > len(moves):
                continue
            if phase > 0:
                for item in moves[phase - 1](q):
                    item.wait_recv()
            works[phase](q)
            if phase < len(moves):
                for item in moves[phase](q):
                    item.start()
    for q in range(chunks):
        for move in moves:
            for item in move(q):
                item.wait_send()


def forward_kernel(
    ah, al, ch, cl, eig_a, eig_c, x_ref,
    z_ref, carry_ref,
    own, other, sums, far, lines, rho, power, up_ref, down_ref, carry,
    own_sem, rep_send, rep_recv, col_send, col_recv,
    *ring,
):
    row = lax.axis_index("row")
    depth = lax.axis_size("row") // 2
    rep = lax.axis_index("rep")
    col = lax.axis_index("col")
    groups, bands, tall, band = own.shape
    slab = tall // GROUP
    count = z_ref.shape[0]
    shift = GROUP // 2

    barrier = pltpu.get_barrier_semaphore()
    peer_signal(barrier, {"rep": 1 - rep})
    peer_signal(barrier, {"col": 1 - col})
    peer_signal(barrier, {"row": row + 1 - 2 * (row % 2)})
    for m in range(1, depth):
        peer_signal(barrier, {"row": (row // 2 + m) % depth * 2 + row % 2})
    pl.semaphore_wait(barrier, 2 + depth)

    def first_line(n, owner):
        chain = 1 - col if n < 2 else col
        start = chain * (2 * count) + (owner + n % 2) * GROUP
        return pl.multiple_of(start, GROUP)

    def rep_copy(n, j):
        start = first_line(n, 1 - rep)
        return send(
            x_ref.at[:, pl.ds(start, GROUP), pl.ds(j * band, band)],
            other.at[n, j].reshape(slab, GROUP, band),
            rep_send.at[n, j],
            rep_recv.at[n, j],
            {"rep": 1 - rep},
        )

    def own_copy(n, j):
        start = first_line(n, rep)
        return pltpu.make_async_copy(
            x_ref.at[:, pl.ds(start, GROUP), pl.ds(j * band, band)],
            own.at[n, j].reshape(slab, GROUP, band),
            own_sem.at[n, j],
        )

    def col_copy(t):
        return send(
            sums.at[0, t],
            far.at[t],
            col_send.at[t],
            col_recv.at[t],
            {"col": 1 - col},
        )

    for n in range(groups):
        for j in range(bands):
            rep_copy(n, j).start()
            own_copy(n, j).start()
    decay, _ = decay_of(eig_a[...] + eig_c[...] + 0.001)
    rho[...] = decay
    power[...] = jnp.ones_like(decay)
    up_ref[...] = jnp.zeros_like(decay)
    down_ref[...] = jnp.zeros_like(decay)

    for n in range(groups):
        for j in range(bands):
            rep_copy(n, j).wait_recv()
            own_copy(n, j).wait()

        def add(s, _):
            t = n % 2 * GROUP + s - shift * rep
            rows = pl.ds(s, slab, stride=GROUP)

            @pl.when((t >= 0) & (t < count))
            def _():
                for j in range(bands):
                    sums[n // 2, t, :, j * band : (j + 1) * band] = (
                        own[n, j, rows, :] + other[n, j, rows, :]
                    )
                if n < 2:
                    col_copy(t).start()

            return 0

        lax.fori_loop(0, GROUP, add, 0)

    def transform(t, _):
        here = pl.ds(pl.multiple_of(col * slab, 8), slab)
        there = pl.ds(pl.multiple_of((1 - col) * slab, 8), slab)
        lines[here, :] = times_table(sums[1, t], ch[...], cl[...])
        col_copy(t).wait_recv()
        lines[there, :] = times_table(far[t], ch[...], cl[...])
        modes = table_times(ah[...], al[...], lines[...])
        z_ref[t] = modes
        up_ref[...] = modes + rho[...] * up_ref[...]
        down_ref[...] = down_ref[...] + power[...] * modes
        power[...] = power[...] * rho[...]
        return 0

    lax.fori_loop(0, count, transform, 0)
    exchange_carries(depth, count, up_ref, down_ref, rho, carry, *ring)
    carry_ref[...] = carry[...]
    for n in range(groups):
        for j in range(bands):
            rep_copy(n, j).wait_send()

    def drain(t, _):
        col_copy(t).wait_send()
        return 0

    lax.fori_loop(0, count, drain, 0)


def backward_kernel(
    scale,
    ah, al, ch, cl, eig_a, eig_c, z_ref, carry,
    out_ref,
    rho, gain, run, back, planes,
    own_sem, send_sem, recv_sem,
):
    rep = lax.axis_index("rep")
    col = lax.axis_index("col")
    count = z_ref.shape[0]
    slab = out_ref.shape[1]
    offsets = ((0, 1), (1, 1), (1, 0))

    barrier = pltpu.get_barrier_semaphore()
    for flip_rep, flip_col in offsets:
        peer_signal(barrier, {"rep": (rep + flip_rep) % 2, "col": (col + flip_col) % 2})
    pl.semaphore_wait(barrier, 3)

    mine = rep * 2 + col
    block = col * 2 + rep

    def peer_copy(k, t):
        to_rep = (rep + offsets[k][0]) % 2
        to_col = (col + offsets[k][1]) % 2
        start = pl.multiple_of((to_rep * 2 + to_col) * slab, 8)
        return send(
            planes.at[t, pl.ds(start, slab), :],
            out_ref.at[block * count + t],
            send_sem.at[k, t],
            recv_sem.at[k, t],
            {"rep": to_rep, "col": to_col},
        )

    def own_copy(t):
        start = pl.multiple_of(mine * slab, 8)
        return pltpu.make_async_copy(
            planes.at[t, pl.ds(start, slab), :], out_ref.at[block * count + t], own_sem.at[t]
        )

    decay, root = decay_of(eig_a[...] + eig_c[...] + 0.001)
    rho[...] = decay
    gain[...] = scale / root
    run[...] = carry[0]
    back[count - 1] = decay * carry[1]

    def down(t, _):
        here = count - 2 - t
        back[here] = rho[...] * (z_ref[here + 1] + back[here + 1])
        return 0

    lax.fori_loop(0, count - 1, down, 0)

    def emit(t, _):
        run[...] = z_ref[t] + rho[...] * run[...]
        field = gain[...] * (run[...] + back[t])
        lines = table_times(ah[...], al[...], field)
        planes[t] = times_table(lines, ch[...], cl[...])
        for k in range(3):
            peer_copy(k, t).start()
        own_copy(t).start()
        return 0

    lax.fori_loop(0, count, emit, 0)

    def drain(t, _):
        own_copy(t).wait()
        for k in range(3):
            peer_copy(k, t).wait()
        return 0

    lax.fori_loop(0, count, drain, 0)


def forward_call(x, tables):
    slab, width, cols = x.shape
    rows = slab * 2
    half = width // 2
    count = half // 2
    carry = jax.ShapeDtypeStruct((2, rows, cols), jnp.float32)
    modes = jax.ShapeDtypeStruct((count, rows, cols), jnp.float32)
    vmem = pl.BlockSpec(memory_space=pltpu.VMEM)
    groups = 4
    depth = lax.axis_size("row") // 2
    tall = depth * 8
    chunks = rows // (4 * tall)
    dma = pltpu.SemaphoreType.DMA
    f32 = jnp.float32
    return pl.pallas_call(
        forward_kernel,
        in_specs=[vmem] * len(tables) + [pl.BlockSpec(memory_space=pl.ANY)],
        out_specs=[vmem] * 2,
        out_shape=[modes, carry],
        scratch_shapes=[
            pltpu.VMEM((groups, cols // LANES, slab * GROUP, LANES), f32),
            pltpu.VMEM((groups, cols // LANES, slab * GROUP, LANES), f32),
            pltpu.VMEM((2, count, slab, cols), f32),
            pltpu.VMEM((count, slab, cols), f32),
        ]
        + [pltpu.VMEM((rows, cols), f32)] * 5
        + [
            pltpu.VMEM((2, rows, cols), f32),
            dma((groups, cols // LANES)),
            dma((groups, cols // LANES)),
            dma((groups, cols // LANES)),
            dma((count,)),
            dma((count,)),
        ]
        + [
            pltpu.VMEM((chunks,) + shape + (cols,), f32)
            for shape in (
                (2, 2 * tall), (2, 2 * tall), (2 * tall,), (2 * tall,), (tall,), (tall,),
                (depth, 8), (depth, 8), (tall,), (tall,), (2 * tall,), (2 * tall,),
                (2, 2 * tall),
            )
        ]
        + [dma((chunks, 6 + 2 * depth))] * 2,
        compiler_params=pltpu.CompilerParams(
            collective_id=0, has_side_effects=True, vmem_limit_bytes=VMEM_BYTES
        ),
    )(*tables, x)


def backward_call(z, carry, tables, scale):
    count, rows, cols = z.shape
    vmem = pl.BlockSpec(memory_space=pltpu.VMEM)
    dma = pltpu.SemaphoreType.DMA
    return pl.pallas_call(
        functools.partial(backward_kernel, scale),
        in_specs=[vmem] * (len(tables) + 2),
        out_specs=pl.BlockSpec(memory_space=pl.ANY),
        out_shape=jax.ShapeDtypeStruct((count * 4, rows // 4, cols), jnp.float32),
        scratch_shapes=[pltpu.VMEM((rows, cols), jnp.float32)] * 3
        + [pltpu.VMEM(z.shape, jnp.float32)] * 2
        + [dma((count,)), dma((3, count)), dma((3, count))],
        compiler_params=pltpu.CompilerParams(
            collective_id=1, has_side_effects=True, vmem_limit_bytes=VMEM_BYTES
        ),
    )(*tables, z, carry)


def line_body(sources):
    partial_value = sources[0]
    slab, width, length_c = partial_value.shape
    length_a = slab * lax.axis_size("col")
    high_a, low_a = slab_tables(length_a)
    high_c, low_c = slab_tables(length_c)
    eig_a = eigen_values(length_a)
    eig_c = eigen_values(length_c)
    tables = (
        high_a,
        low_a,
        high_c,
        low_c,
        jnp.asarray(eig_a)[:, None],
        jnp.asarray(eig_c)[None, :],
    )
    modes, carry = forward_call(partial_value, tables)
    result = backward_call(modes, carry, tables, 1.0 / (length_a * length_c))
    return result.transpose(1, 0, 2)


def solution(mesh):
    in_specs = (P("rep", "col", "row", None),)
    out_specs = P(("rep", "col"), "row", None)
    pairs = mesh.shape["rep"] == 2 and mesh.shape["col"] == 2
    rows = mesh.shape["row"]
    split_lines = pairs and rows % 2 == 0 and NB == rows * 6 * GROUP
    split_lines = split_lines and NA % (16 * rows) == 0 and NC % LANES == 0
    chosen = line_body if split_lines else body
    return jax.shard_map(chosen, mesh=mesh, in_specs=in_specs, out_specs=out_specs, check_vma=False)
```
